256 devices in a mesh: seg: 4 (over x_lo, core), ops: 64 (over x_hi, y, z).
Axes of the slice: x: 4 (x_hi: 2, x_lo: 2; x = x_hi * 2 + x_lo), y: 4, z: 8, core: 2. Of those that a mesh axis runs over, the one named last changes fastest.
Arguments:
- amat: bfloat16 [16384, 128], P(('seg', 'ops')), may hold values from -6 to 6
- lam: float32 [16384], P(('seg', 'ops')), may hold values from 0.3 to 3
- hdiag: float32 [16384, 128], P(('seg', 'ops')), may hold values from 0.25 to 8
- left_ops: bfloat16 [4, 384, 4096, 128], P('seg', 'ops'), may hold values from -0.5 to 0.5
- right_operators: bfloat16 [4, 384, 4096, 128], P('seg', 'ops'), may hold values from -0.02734375 to 0.02734375
- couple: int32 [4, 384, 32], P('seg', 'ops'), may hold values from 0 to 31
- blockmask: int32 [4, 384, 32], P('seg', 'ops'), may hold values 0 or 1
Outputs:
- sigma_two: float32 [16384, 128], P(('seg', 'ops'))
- theta: float32 [4], P('seg')
The draws below stay inside these ranges and needn't reach their ends.
Inputs may be any that keep to these rules, and one draw needn't show every extreme that they name: couple[s, k, i] is the sector of the vector that term k of segment s carries into sector i.
All inputs are finite; a program needn't handle non-finite values. No bound on the sum of `blockmask` on one device may be relied on, other than what follows from the above.
Results may differ from the reference program's by a relative error of at most 0.009.
Values may be sent and summed in bfloat16 or wider, within the bound.
A program may use at most 64 MiB of HBM per device.

```python
import math
import jax
import jax.numpy as jnp
from jax import lax

M = 4096
NQ = 32
BS = 128
TERMS = 384
SEGS = 4
N_SEG = 4


def draw_hdiag(key, part):
    noise_key = jax.random.fold_in(key, 11)
    row_index = jnp.arange(SEGS * M, dtype=jnp.int32) % M
    segment_position = row_index.astype(jnp.float32) / (M - 1)
    incline = jnp.power(3.0, segment_position)
    texture = jnp.exp(jax.random.uniform(noise_key, (SEGS * M, BS), jnp.float32, -math.log(2.0), math.log(2.0)))
    return (0.5 * incline[:, None] * texture).astype(jnp.float32)


def place_ends(entries, key, smallest, largest):
    place = [jax.random.randint(jax.random.fold_in(key, axis), (), 0, length) for axis, length in enumerate(entries.shape)]
    longest = entries.shape.index(max(entries.shape))
    beside = place[:longest] + [(place[longest] + 1) % entries.shape[longest]] + place[longest + 1:]
    return entries.at[tuple(place)].set(smallest).at[tuple(beside)].set(largest)


def level_of(stream_key, extent, shards, low, largest):
    gain = 1.0
    for axis_at, shards_of in shards:
        draws = jax.random.uniform(jax.random.fold_in(jax.random.fold_in(stream_key, 6), axis_at), (shards_of,), jnp.float32, low / len(shards), largest / len(shards))
        gain = gain * jnp.repeat(jnp.exp(draws), extent[axis_at] // shards_of).reshape((-1,) + (1,) * (len(extent) - 1 - axis_at))
    return gain


def normal_values(rng, dims, spread, reach, shards=(), held_as=jnp.bfloat16):
    result = spread * jax.random.normal(rng, dims, jnp.float32)
    if shards:
        result = result * level_of(rng, dims, shards, -0.22, 0.18)
    return jnp.clip(result, -reach, reach).astype(held_as)


def setup_inputs(seed: int = 0) -> dict:
    key_of = jax.random.split(jax.random.key(seed), 8)
    amat = normal_values(key_of[0], (SEGS * M, BS), 1.0, 6.0, ((0, 256),))
    lam = jnp.clip(jnp.exp(math.log(3.0) - 2.3025851 * jax.random.uniform(key_of[1], (SEGS * M,), jnp.float32) ** level_of(key_of[1], (SEGS * M,), ((0, 256),), -0.2, 0.2)), 0.3, 3.0)
    hdiag = draw_hdiag(jax.random.fold_in(key_of[7], 71), 0)
    left_ops = normal_values(key_of[3], (SEGS, TERMS, M, BS), BS ** -0.5, 0.5, ((0, 4), (1, 64)))
    right_operators = normal_values(key_of[4], (SEGS, TERMS, M, BS), (BS * TERMS) ** -0.5, 0.02734375, ((0, 4), (1, 64)))
    couple = place_ends(jax.random.randint(key_of[5], (SEGS, TERMS, NQ), 0, NQ), jax.random.fold_in(key_of[5], 1), 0, NQ - 1).astype(jnp.int32)
    blockmask = place_ends((jax.random.randint(key_of[6], (SEGS, TERMS, NQ), 0, 4) < 3).astype(jnp.int32), jax.random.fold_in(key_of[6], 1), 0, 1)
    return dict(amat=amat, lam=lam, hdiag=hdiag, left_ops=left_ops, right_operators=right_operators, couple=couple, blockmask=blockmask)


def apply_terms(vector, diagonal_entries, left, right, links, live):
    blocks = vector.reshape(NQ, BS, BS).astype(jnp.float32)

    def step(total_sum, index):
        picked = blocks[links[index]]
        lblk = left[index].reshape(NQ, BS, BS).astype(jnp.float32)
        inner_block = jnp.einsum('iab,ibc->iac', lblk, picked)
        inner_block = inner_block * live[index].astype(jnp.float32)[:, None, None]
        inner_block = inner_block.astype(jnp.bfloat16).astype(jnp.float32)
        right_block = right[index].reshape(NQ, BS, BS).astype(jnp.float32)
        return total_sum + jnp.einsum('nwr,nzr->nwz', inner_block, right_block), None

    start = jnp.zeros((NQ, BS, BS), jnp.float32)
    total_sum, unused = lax.scan(step, start, jnp.arange(TERMS, dtype=jnp.int32))
    return total_sum.reshape(M, BS) + diagonal_entries * vector.astype(jnp.float32)


def reference(amat, lam, hdiag, left_ops, right_operators, couple, blockmask):
    output_blocks = []
    quotients = []
    for segment in range(N_SEG):
        lower = segment * M
        upper = lower + M
        tensor = amat[lower:upper].astype(jnp.float32)
        if segment == 0:
            weights = jnp.ones((M,), jnp.float32)
        else:
            weights = lam[lower - M:lower]
        psi = (weights[:, None] * tensor).astype(jnp.bfloat16)
        diagonal_entries = hdiag[lower:upper]
        left = left_ops[segment]
        right = right_operators[segment]
        links = couple[segment]
        live = blockmask[segment]
        sigma_one = apply_terms(psi, diagonal_entries, left, right, links, live)
        psi_float = psi.astype(jnp.float32)
        quotient = jnp.sum(psi_float * sigma_one) / jnp.sum(psi_float * psi_float)
        correction = ((sigma_one - quotient * psi_float) / diagonal_entries).astype(jnp.bfloat16)
        output_blocks.append(apply_terms(correction, diagonal_entries, left, right, links, live))
        quotients.append(quotient)
    return jnp.concatenate(output_blocks, axis=0), jnp.stack(quotients)
```

```python
import functools

import jax
import jax.numpy as jnp
from jax import lax
from jax.experimental import pallas as pl
from jax.experimental.pallas import tpu as pltpu
from jax.sharding import PartitionSpec as P

NX, NY, NZ = 2, 4, 8
NXZ = NX * NZ
NSEG = 4
NQ, BS, ROWS = 32, 128, 64
UNIT = 4
LAG = 6
F32, BF16 = jnp.float32, jnp.bfloat16


def kernel(amat_h, lam_h, hdiag_h, left_h, right_h, couple, mask,
           out, theta_out,
           amat, lam, hdiag, left, right, lam_in, v, opp_send, near_send,
           opp_in, near_in, own_acc, plane_send, plane_in, sigma,
           numer, denom, numer_y, numer_p,
           load_sem, lam_sem, op_sem, lam_send, plane_s, plane_r,
           ring_s, ring_r, last_s, last_r, sum_s, sum_r, psum_s, psum_r,
           num_s, num_r, nump_s, nump_r):
    nterms = left.shape[0]
    seg = lax.axis_index("seg")
    me = lax.axis_index("ops")
    x, y, z = me // (NY * NZ), (me // NZ) % NY, me % NZ
    xz = x * NZ + z
    up, down, across = (y + 1) % NY, (y + 3) % NY, (y + 2) % NY

    def device(tx, ty, tz):
        return tx * (NY * NZ) + ty * NZ + tz

    def place(p):
        q = p // 2
        dz = (q % 2) * ((q + 1) // 2) + (1 - q % 2) * (NZ - q // 2)
        return (x + p) % NX, (z + dz) % NZ

    def piece(ref, o):
        return ref.at[o // 2, pl.ds(pl.multiple_of((o % 2) * ROWS, ROWS), ROWS), :]

    def remote(src, dst, s, r, target, axis="ops"):
        return pltpu.make_async_remote_copy(
            src_ref=src, dst_ref=dst, send_sem=s, recv_sem=r,
            device_id={axis: target}, device_id_type=pl.DeviceIdType.MESH)

    small = [pltpu.make_async_copy(amat_h, amat, load_sem.at[0]),
             pltpu.make_async_copy(lam_h, lam, load_sem.at[1]),
             pltpu.make_async_copy(hdiag_h, hdiag, load_sem.at[2])]
    for copy in small:
        copy.start()

    def operator_copies(k):
        return (pltpu.make_async_copy(left_h.at[k], left.at[k], op_sem.at[0, k]),
                pltpu.make_async_copy(right_h.at[k], right.at[k], op_sem.at[1, k]))

    for k in range(nterms):
        for copy in operator_copies(k):
            copy.start()

    barrier = pltpu.get_barrier_semaphore()

    def greet(p, c):
        tx, tz = place(p)
        pl.semaphore_signal(barrier, inc=1, device_id={"ops": device(tx, y, tz)},
                            device_id_type=pl.DeviceIdType.MESH)
        return c

    lax.fori_loop(1, NXZ, greet, 0)
    for other in (up, down, across):
        pl.semaphore_signal(barrier, inc=1, device_id={"ops": device(x, other, z)},
                            device_id_type=pl.DeviceIdType.MESH)
    for step in (1, NSEG - 1):
        pl.semaphore_signal(barrier, inc=1, device_id={"seg": (seg + step) % NSEG},
                            device_id_type=pl.DeviceIdType.MESH)
    for copy in small:
        copy.wait()
    v[0, NQ] = jnp.zeros((BS, BS), BF16)
    v[1, NQ] = jnp.zeros((BS, BS), BF16)
    numer[...] = jnp.zeros_like(numer)
    denom[...] = jnp.zeros_like(denom)
    pl.semaphore_wait(barrier, NXZ - 1 + 3 + 2)

    pass_lam = remote(lam, lam_in, lam_send, lam_sem, (seg + 1) % NSEG, "seg")
    pass_lam.start()
    pass_lam.wait_recv()
    square = (ROWS, ROWS)
    diagonal = lax.broadcasted_iota(jnp.int32, square, 0) == lax.broadcasted_iota(jnp.int32, square, 1)
    earlier = jnp.sum(jnp.where(diagonal, jnp.broadcast_to(lam_in[...], square), 0.0), axis=1, keepdims=True)
    weights = jnp.where(seg == 0, jnp.ones_like(earlier), earlier)
    psi = (weights * amat[...].astype(F32)).astype(BF16)

    mine = (me // 2, pl.ds(pl.multiple_of((me % 2) * ROWS, ROWS), ROWS))

    def gather(s, value):
        vec = v.at[s]
        v[s, mine[0], mine[1], :] = value

        def scatter_copy(p):
            tx, tz = place(p)
            return remote(piece(vec, me), piece(vec, me), plane_s.at[p], plane_r.at[s, xz],
                          device(tx, y, tz))

        def arrival(p, ty, sem):
            tx, tz = place(p)
            where = piece(vec, device(tx, ty, tz))
            return remote(where, where, plane_s.at[p], sem.at[s, tx * NZ + tz], device(x, up, z))

        def pass_up(p):
            tx, tz = place(p)
            where = piece(vec, device(tx, y, tz))
            return remote(where, where, ring_s.at[0, p], ring_r.at[0, s, tx * NZ + tz], device(x, up, z))

        def pass_down(p):
            tx, tz = place(p)
            where = piece(vec, device(tx, y, tz))
            return remote(where, where, ring_s.at[1, p], ring_r.at[1, s, tx * NZ + tz], device(x, down, z))

        def on_up(p):
            tx, tz = place(p)
            where = piece(vec, device(tx, down, tz))
            return remote(where, where, last_s.at[p], last_r.at[s, tx * NZ + tz], device(x, up, z))

        def on_down(p):
            tx, tz = place(p)
            where = piece(vec, device(tx, up, tz))
            return remote(where, where, last_s.at[p], last_r.at[s, tx * NZ + tz], device(x, down, z))

        def first(p, c):
            scatter_copy(p).start()
            return c

        lax.fori_loop(1, NXZ, first, 0)

        def hop(p, c):
            @pl.when(p < NXZ)
            def _():
                @pl.when(p > 0)
                def _():
                    arrival(p, y, plane_r).wait_recv()
                pass_up(p).start()
                pass_down(p).start()

            @pl.when(p >= LAG)
            def _():
                q = p - LAG

                @pl.when((q // 2) % 2 == 0)
                def _():
                    arrival(q, down, ring_r.at[0]).wait_recv()
                    on_up(q).start()

                @pl.when((q // 2) % 2 == 1)
                def _():
                    arrival(q, up, ring_r.at[1]).wait_recv()
                    on_down(q).start()
            return c

        lax.fori_loop(0, NXZ + LAG, hop, 0)

        def finish(p, c):
            @pl.when((p // 2) % 2 == 0)
            def _():
                arrival(p, up, ring_r.at[1]).wait_recv()

            @pl.when((p // 2) % 2 == 1)
            def _():
                arrival(p, down, ring_r.at[0]).wait_recv()

            arrival(p, across, last_r).wait_recv()
            return c

        lax.fori_loop(0, NXZ, finish, 0)

        def sent(p, c):
            @pl.when(p > 0)
            def _():
                scatter_copy(p).wait_send()
            pass_up(p).wait_send()
            pass_down(p).wait_send()
            on_up(p).wait_send()
            return c

        return functools.partial(lax.fori_loop, 0, NXZ, sent, 0)

    contract = (((1,), (1,)), ((), ()))

    def block(s, i):
        inner = []
        for k in range(nterms):
            live = mask[k, i]
            j = couple[k, i] * live + NQ * (1 - live)
            inner.append(jnp.dot(left[k, i], v[s, j], preferred_element_type=F32).astype(BF16))
        total = None
        for k in range(0, nterms, 2):
            pair = jnp.concatenate(inner[k:k + 2], axis=1)
            rpair = jnp.concatenate([right[k, i], right[k + 1, i]], axis=1)
            part = lax.dot_general(pair, rpair, contract, preferred_element_type=F32)
            total = part if total is None else total + part
        if s == 0:
            here = v[s, i].astype(F32)
            numer[...] += jnp.sum((total * here).reshape(BS // 8, 8, BS), axis=0)
            denom[...] += jnp.sum((here * here).reshape(BS // 8, 8, BS), axis=0)
        return total

    def unit(s, half, ty, keep):
        base = half * (NQ // 2) + ty * UNIT

        def step(b, c):
            for b2 in range(2):
                keep(2 * b + b2, block(s, base + 2 * b + b2))
            return c

        lax.fori_loop(0, UNIT // 2, step, 0)

    def reduce(s):
        sends = []

        def send(src, dst, index, target):
            copy = remote(src, dst, sum_s.at[index], sum_r.at[s, index], device(x, target, z))
            copy.start()
            sends.append(copy)

        def got(dst, index):
            remote(dst, dst, sum_s.at[index], sum_r.at[s, index], device(x, up, z)).wait_recv()

        def to(ref, *at):
            def keep(b, total):
                ref[(*at, b)] = total.astype(ref.dtype)
            return keep

        def plus(ref, add, at, add_at):
            def keep(b, total):
                ref[(*at, b)] = (total + add[(*add_at, b)].astype(F32)).astype(ref.dtype)
            return keep

        unit(s, 0, across, to(opp_send, 0))
        send(opp_send.at[0], opp_in.at[s, 0], 0, up)
        unit(s, 1, across, to(opp_send, 1))
        send(opp_send.at[1], opp_in.at[s, 1], 1, down)
        unit(s, 1, up, to(near_send, 0, 1))
        send(near_send.at[0, 1], near_in.at[s, 0, 1], 2, up)
        unit(s, 0, down, to(near_send, 1, 0))
        send(near_send.at[1, 0], near_in.at[s, 1, 0], 3, down)
        got(opp_in.at[s, 0], 0)
        unit(s, 0, up, plus(near_send, opp_in, (0, 0), (s, 0)))
        send(near_send.at[0, 0], near_in.at[s, 0, 0], 4, up)
        got(opp_in.at[s, 1], 1)
        unit(s, 1, down, plus(near_send, opp_in, (1, 1), (s, 1)))
        send(near_send.at[1, 1], near_in.at[s, 1, 1], 5, down)
        unit(s, 0, y, to(own_acc, 0))
        unit(s, 1, y, to(own_acc, 1))

        if s == 0:
            own = psi.astype(F32)
            numer[...] += jnp.sum((hdiag[...] * own * own).reshape(ROWS // 8, 8, BS), axis=0)
            numer_y[y] = numer[...]
            for n, other in enumerate((up, down, across)):
                copy = remote(numer, numer_y.at[y], num_s.at[n], num_r.at[y], device(x, other, z))
                copy.start()
                sends.append(copy)

        def plane_copy(half, t):
            o = half * NZ + t
            return remote(plane_send.at[half, t], plane_in.at[s, xz], psum_s.at[o], psum_r.at[s, xz],
                          device(half, y, t))

        for half in range(2):
            got(near_in.at[s, 0, half], 4 if half == 0 else 2)
            got(near_in.at[s, 1, half], 3 if half == 0 else 5)

            def add(b, c):
                total = (own_acc[half, b] + near_in[s, 0, half, b].astype(F32)
                         + near_in[s, 1, half, b].astype(F32))
                own_acc[half, b] = total
                plane_send[half, 2 * b] = total[:ROWS].astype(BF16)
                plane_send[half, 2 * b + 1] = total[ROWS:].astype(BF16)
                return c

            lax.fori_loop(0, UNIT, add, 0)

            def go(t, c):
                @pl.when(half * NZ + t != xz)
                def _():
                    plane_copy(half, t).start()
                return c

            lax.fori_loop(0, NZ, go, 0)

        if s == 0:
            for other in (up, down, across):
                remote(numer, numer_y.at[other], num_s.at[0], num_r.at[other], device(x, up, z)).wait_recv()
            numer_p[xz] = (numer_y[0] + numer_y[1]) + (numer_y[2] + numer_y[3])

            def numer_copy(p):
                tx, tz = place(p)
                return remote(numer_p.at[xz], numer_p.at[xz], nump_s.at[p], nump_r.at[xz], device(tx, y, tz))

            def go_numer(p, c):
                numer_copy(p).start()
                return c

            lax.fori_loop(1, NXZ, go_numer, 0)

        sigma[...] = own_acc[x, z // 2, pl.ds(pl.multiple_of((z % 2) * ROWS, ROWS), ROWS), :]

        def take(p, c):
            tx, tz = place(p)
            o = tx * NZ + tz
            remote(plane_in.at[s, o], plane_in.at[s, o], psum_s.at[0], psum_r.at[s, o],
                   device(x, up, z)).wait_recv()
            sigma[...] += plane_in[s, o].astype(F32)
            return c

        lax.fori_loop(1, NXZ, take, 0)

        if s == 0:
            def take_numer(p, c):
                tx, tz = place(p)
                o = tx * NZ + tz
                remote(numer_p.at[o], numer_p.at[o], nump_s.at[0], nump_r.at[o], device(x, up, z)).wait_recv()
                return c

            lax.fori_loop(1, NXZ, take_numer, 0)

        def drain():
            for copy in sends:
                copy.wait_send()

            def sent(o, c):
                @pl.when(o != xz)
                def _():
                    plane_copy(o // NZ, o % NZ).wait_send()
                return c

            lax.fori_loop(0, NXZ, sent, 0)
            if s == 0:
                def sent_numer(p, c):
                    numer_copy(p).wait_send()
                    return c

                lax.fori_loop(1, NXZ, sent_numer, 0)

        return drain

    sent_psi = gather(0, psi)
    for k in range(nterms):
        for copy in operator_copies(k):
            copy.wait()
    drain_one = reduce(0)
    psi_float = psi.astype(F32)
    sigma_one = sigma[...] + hdiag[...] * psi_float
    top = jnp.sum(jnp.sum(numer_p[...], axis=0), keepdims=True)
    quotient = top / jnp.sum(denom[...], keepdims=True)
    correction = ((sigma_one - quotient * psi_float) / hdiag[...]).astype(BF16)
    sent_psi()
    sent_correction = gather(1, correction)
    drain_one()
    theta_out[0] = quotient[0, 0]
    pass_lam.wait_send()
    drain_two = reduce(1)
    out[...] = sigma[...] + hdiag[...] * correction.astype(F32)
    sent_correction()
    drain_two()


def body(amat, lam, hdiag, left_ops, right_operators, couple, blockmask):
    terms = left_ops.shape[1]
    vmem, dma = pltpu.VMEM, pltpu.SemaphoreType.DMA
    anywhere = pl.BlockSpec(memory_space=pl.ANY)
    scalars = pl.BlockSpec(memory_space=pltpu.SMEM)
    scratch = [
        vmem((ROWS, BS), BF16), vmem((1, ROWS), F32), vmem((ROWS, BS), F32),
        vmem((terms, NQ, BS, BS), BF16), vmem((terms, NQ, BS, BS), BF16),
        vmem((1, ROWS), F32),
        vmem((2, NQ + 1, BS, BS), BF16),
        vmem((2, UNIT, BS, BS), BF16), vmem((2, 2, UNIT, BS, BS), BF16),
        vmem((2, 2, UNIT, BS, BS), BF16), vmem((2, 2, 2, UNIT, BS, BS), BF16),
        vmem((2, UNIT, BS, BS), F32),
        vmem((2, NZ, ROWS, BS), BF16), vmem((2, NXZ, ROWS, BS), BF16),
        vmem((ROWS, BS), F32),
        vmem((8, BS), F32), vmem((8, BS), F32),
        vmem((NY, 8, BS), F32), vmem((NXZ, 8, BS), F32),
        dma((3,)), dma, dma((2, terms)), dma,
        dma((NXZ,)), dma((2, NXZ)),
        dma((2, NXZ)), dma((2, 2, NXZ)),
        dma((NXZ,)), dma((2, NXZ)),
        dma((6,)), dma((2, 6)),
        dma((NXZ,)), dma((2, NXZ)),
        dma((3,)), dma((NY,)),
        dma((NXZ,)), dma((NXZ,)),
    ]
    sigma_two, theta = pl.pallas_call(
        kernel,
        out_shape=(jax.ShapeDtypeStruct((ROWS, BS), F32), jax.ShapeDtypeStruct((1,), F32)),
        in_specs=[anywhere] * 5 + [scalars] * 2,
        out_specs=(pl.BlockSpec(memory_space=pltpu.VMEM), scalars),
        scratch_shapes=scratch,
        compiler_params=pltpu.CompilerParams(collective_id=0, has_side_effects=True),
    )(amat, lam.reshape(1, ROWS), hdiag,
      left_ops.reshape(terms, NQ, BS, BS), right_operators.reshape(terms, NQ, BS, BS),
      couple[0], blockmask[0])
    return sigma_two, theta


def solution(mesh):
    placed = (
        P(("seg", "ops"), None),
        P(("seg", "ops")),
        P(("seg", "ops"), None),
        P("seg", "ops", None, None),
        P("seg", "ops", None, None),
        P("seg", "ops", None),
        P("seg", "ops", None),
    )
    return jax.shard_map(
        body,
        mesh=mesh,
        in_specs=placed,
        out_specs=(P(("seg", "ops"), None), P("seg")),
        check_vma=False,
    )
```

```python
import functools

import jax
import jax.numpy as jnp
from jax import lax
from jax.experimental import pallas as pl
from jax.experimental.pallas import tpu as pltpu
from jax.sharding import PartitionSpec as P

NX, NY, NZ = 2, 4, 8
NXZ = NX * NZ
NSEG = 4
NQ, BS, ROWS = 32, 128, 64
UNIT = GROUPS = 4
F32, BF16 = jnp.float32, jnp.bfloat16


def kernel(amat_h, lam_h, hdiag_h, left_h, right_h, couple, mask,
           out, theta_out,
           amat, lam, hdiag, left, right, lam_in, v, opp_send, near_send,
           opp_in, near_in, own_acc, work, plane_send, plane_in, sigma,
           numer, denom, numer_y, numer_p,
           load_sem, lam_sem, op_sem, lam_send, plane_s, plane_r,
           ring_s, ring_r, opp_s, opp_r, near_s, near_r, psum_s, psum_r,
           num_s, num_r, nump_s, nump_r):
    nterms = left.shape[0]
    seg = lax.axis_index("seg")
    me = lax.axis_index("ops")
    x, y, z = me // (NY * NZ), (me // NZ) % NY, me % NZ
    xz = x * NZ + z
    up, down, across = (y + 1) % NY, (y + 3) % NY, (y + 2) % NY

    def device(tx, ty, tz):
        return tx * (NY * NZ) + ty * NZ + tz

    def place(p):
        q = p // 2
        dz = (q % 2) * ((q + 1) // 2) + (1 - q % 2) * (NZ - q // 2)
        return (x + p) % NX, (z + dz) % NZ

    def piece(ref, o):
        return ref.at[o // 2, pl.ds(pl.multiple_of((o % 2) * ROWS, ROWS), ROWS), :]

    def remote(src, dst, s, r, target, axis="ops"):
        return pltpu.make_async_remote_copy(
            src_ref=src, dst_ref=dst, send_sem=s, recv_sem=r,
            device_id={axis: target}, device_id_type=pl.DeviceIdType.MESH)

    small = [pltpu.make_async_copy(amat_h, amat, load_sem.at[0]),
             pltpu.make_async_copy(lam_h, lam, load_sem.at[1]),
             pltpu.make_async_copy(hdiag_h, hdiag, load_sem.at[2])]
    for copy in small:
        copy.start()

    def operator_copies(k):
        return (pltpu.make_async_copy(left_h.at[k], left.at[k], op_sem.at[0, k]),
                pltpu.make_async_copy(right_h.at[k], right.at[k], op_sem.at[1, k]))

    for k in range(nterms):
        for copy in operator_copies(k):
            copy.start()

    barrier = pltpu.get_barrier_semaphore()

    def greet(p, c):
        tx, tz = place(p)
        pl.semaphore_signal(barrier, inc=1, device_id={"ops": device(tx, y, tz)},
                            device_id_type=pl.DeviceIdType.MESH)
        return c

    lax.fori_loop(1, NXZ, greet, 0)
    for other in (up, down, across):
        pl.semaphore_signal(barrier, inc=1, device_id={"ops": device(x, other, z)},
                            device_id_type=pl.DeviceIdType.MESH)
    for step in (1, NSEG - 1):
        pl.semaphore_signal(barrier, inc=1, device_id={"seg": (seg + step) % NSEG},
                            device_id_type=pl.DeviceIdType.MESH)
    for copy in small:
        copy.wait()
    v[0, NQ] = jnp.zeros((BS, BS), BF16)
    v[1, NQ] = jnp.zeros((BS, BS), BF16)
    numer[...] = jnp.zeros_like(numer)
    denom[...] = jnp.zeros_like(denom)
    pl.semaphore_wait(barrier, NXZ - 1 + 3 + 2)

    pass_lam = remote(lam, lam_in, lam_send, lam_sem, (seg + 1) % NSEG, "seg")
    pass_lam.start()
    pass_lam.wait_recv()
    square = (ROWS, ROWS)
    diagonal = lax.broadcasted_iota(jnp.int32, square, 0) == lax.broadcasted_iota(jnp.int32, square, 1)
    earlier = jnp.sum(jnp.where(diagonal, jnp.broadcast_to(lam_in[...], square), 0.0), axis=1, keepdims=True)
    weights = jnp.where(seg == 0, jnp.ones_like(earlier), earlier)
    psi = (weights * amat[...].astype(F32)).astype(BF16)

    mine = (me // 2, pl.ds(pl.multiple_of((me % 2) * ROWS, ROWS), ROWS))

    def gather(s, value):
        vec = v.at[s]
        v[s, mine[0], mine[1], :] = value

        def scatter_copy(p):
            tx, tz = place(p)
            return remote(piece(vec, me), piece(vec, me), plane_s.at[p], plane_r.at[s, xz],
                          device(tx, y, tz))

        def arrival(p, ty, sem):
            tx, tz = place(p)
            where = piece(vec, device(tx, ty, tz))
            return remote(where, where, plane_s.at[p], sem.at[s, tx * NZ + tz], device(x, up, z))

        def pass_up(p):
            tx, tz = place(p)
            where = piece(vec, device(tx, y, tz))
            return remote(where, where, ring_s.at[0, p], ring_r.at[0, s, tx * NZ + tz], device(x, up, z))

        def pass_down(p):
            tx, tz = place(p)
            where = piece(vec, device(tx, y, tz))
            return remote(where, where, ring_s.at[1, p], ring_r.at[1, s, tx * NZ + tz], device(x, down, z))

        def pass_across(p):
            tx, tz = place(p)
            where = piece(vec, device(tx, y, tz))
            return remote(where, where, ring_s.at[2, p], ring_r.at[2, s, tx * NZ + tz], device(x, across, z))

        def first(p, c):
            scatter_copy(p).start()
            return c

        lax.fori_loop(1, NXZ, first, 0)

        def hop(p, c):
            @pl.when(p > 0)
            def _():
                arrival(p, y, plane_r).wait_recv()
            pass_up(p).start()
            pass_down(p).start()
            pass_across(p).start()
            return c

        lax.fori_loop(0, NXZ, hop, 0)

        def finish(p, c):
            arrival(p, down, ring_r.at[0]).wait_recv()
            arrival(p, up, ring_r.at[1]).wait_recv()
            arrival(p, across, ring_r.at[2]).wait_recv()
            return c

        lax.fori_loop(0, NXZ, finish, 0)

        def sent(p, c):
            @pl.when(p > 0)
            def _():
                scatter_copy(p).wait_send()
            pass_up(p).wait_send()
            pass_down(p).wait_send()
            pass_across(p).wait_send()
            return c

        return functools.partial(lax.fori_loop, 0, NXZ, sent, 0)

    contract = (((1,), (1,)), ((), ()))

    def block(s, i):
        inner = []
        for k in range(nterms):
            live = mask[k, 0, i]
            j = couple[k, 0, i] * live + NQ * (1 - live)
            inner.append(jnp.dot(left[k, i], v[s, j], preferred_element_type=F32).astype(BF16))
        total = None
        for k in range(0, nterms, 2):
            pair = jnp.concatenate(inner[k:k + 2], axis=1)
            rpair = jnp.concatenate([right[k, i], right[k + 1, i]], axis=1)
            part = lax.dot_general(pair, rpair, contract, preferred_element_type=F32)
            total = part if total is None else total + part
        if s == 0:
            here = v[s, i].astype(F32)
            numer[...] += jnp.sum((total * here).reshape(BS // 8, 8, BS), axis=0)
            denom[...] += jnp.sum((here * here).reshape(BS // 8, 8, BS), axis=0)
        return total

    def block_of(half, ty, g):
        return half * (NQ // 2) + ty * UNIT + (z // 2 + (2 - g) * (g < 2) + 3 * (g == 2)) % UNIT

    def unit(s, ty, g):
        return [block(s, block_of(half, ty, g)) for half in range(NX)]

    def reduce(s):
        def opp_copy(g):
            target = device(x, (y + 1 + 2 * (g % 2)) % NY, z)
            return remote(opp_send.at[g], opp_in.at[s, g], opp_s.at[g], opp_r.at[s, g], target)

        def near_copy(d, g):
            target = device(x, (y + 1 + 2 * d) % NY, z)
            return remote(near_send.at[d, g], near_in.at[s, d, g], near_s.at[d, g], near_r.at[s, d, g], target)

        def opposite(n, c):
            groups = (2 * n, 2 * n + 1)
            totals = [unit(s, across, g) for g in groups]
            for g, both in zip(groups, totals):
                for half in range(NX):
                    opp_send[g, half] = both[half].astype(BF16)
                opp_copy(g).start()
            return c

        lax.fori_loop(0, GROUPS // 2, opposite, 0)

        def passed(g):
            d = g % 2
            opp_copy(g).wait_recv()
            for half in range(NX):
                near_send[d, g, half] = (work[d, g, half] + opp_in[s, g, half].astype(F32)).astype(BF16)
            near_copy(d, g).start()

        def near(g, c):
            totals = [unit(s, other, g) for other in (up, down)]
            for d in range(2):
                for half in range(NX):
                    work[d, g, half] = totals[d][half]
            d = 1 - g % 2
            for half in range(NX):
                near_send[d, g, half] = work[d, g, half].astype(BF16)
            near_copy(d, g).start()

            @pl.when(g >= 2)
            def _():
                passed(g - 2)
            return c

        lax.fori_loop(0, GROUPS, near, 0)

        def plane_copy(o):
            return remote(plane_send.at[o], plane_in.at[s, xz], psum_s.at[o], psum_r.at[s, xz],
                          device(o // NZ, y, o % NZ))

        def pass_on(g):
            for d in range(2):
                near_copy(d, g).wait_recv()
            first = block_of(0, 0, g)
            for half in range(NX):
                total = own_acc[g, half] + near_in[s, 0, g, half].astype(F32) + near_in[s, 1, g, half].astype(F32)
                own_acc[g, half] = total
                for side in range(2):
                    plane_send[half * NZ + 2 * first + side] = total[side * ROWS:(side + 1) * ROWS].astype(BF16)
            for half in range(NX):
                for side in range(2):
                    o = half * NZ + 2 * first + side

                    @pl.when(o != xz)
                    def _():
                        plane_copy(o).start()

        def own(n, c):
            groups = (2 * n, 2 * n + 1)
            totals = [unit(s, y, g) for g in groups]
            for g, both in zip(groups, totals):
                for half in range(NX):
                    own_acc[g, half] = both[half]
            passed(2 + n)
            return c

        lax.fori_loop(0, GROUPS // 2, own, 0)

        sends = []
        if s == 0:
            start = psi.astype(F32)
            numer[...] += jnp.sum((hdiag[...] * start * start).reshape(ROWS // 8, 8, BS), axis=0)
            numer_y[y] = numer[...]
            for n, other in enumerate((up, down, across)):
                copy = remote(numer, numer_y.at[y], num_s.at[n], num_r.at[y], device(x, other, z))
                copy.start()
                sends.append(copy)

        lax.fori_loop(0, GROUPS // 2, lambda g, c: (pass_on(g), c)[1], 0)

        if s == 0:
            for other in (up, down, across):
                remote(numer, numer_y.at[other], num_s.at[0], num_r.at[other], device(x, up, z)).wait_recv()
            numer_p[xz] = (numer_y[0] + numer_y[1]) + (numer_y[2] + numer_y[3])

            def numer_copy(p):
                tx, tz = place(p)
                return remote(numer_p.at[xz], numer_p.at[xz], nump_s.at[p], nump_r.at[xz], device(tx, y, tz))

            def go_numer(p, c):
                numer_copy(p).start()
                return c

            lax.fori_loop(1, NXZ, go_numer, 0)

        lax.fori_loop(GROUPS // 2, GROUPS, lambda g, c: (pass_on(g), c)[1], 0)

        sigma[...] = own_acc[GROUPS - 1, x, pl.ds(pl.multiple_of((z % 2) * ROWS, ROWS), ROWS), :]

        def take(p, c):
            tx, tz = place(p)
            o = tx * NZ + tz
            remote(plane_in.at[s, o], plane_in.at[s, o], psum_s.at[0], psum_r.at[s, o],
                   device(x, up, z)).wait_recv()
            sigma[...] += plane_in[s, o].astype(F32)
            return c

        lax.fori_loop(1, NXZ, take, 0)

        if s == 0:
            def take_numer(p, c):
                tx, tz = place(p)
                o = tx * NZ + tz
                remote(numer_p.at[o], numer_p.at[o], nump_s.at[0], nump_r.at[o], device(x, up, z)).wait_recv()
                return c

            lax.fori_loop(1, NXZ, take_numer, 0)

        def drain():
            for copy in sends:
                copy.wait_send()

            def sent_ring(g, c):
                opp_copy(g).wait_send()
                near_copy(0, g).wait_send()
                near_copy(1, g).wait_send()
                return c

            lax.fori_loop(0, GROUPS, sent_ring, 0)

            def sent(o, c):
                @pl.when(o != xz)
                def _():
                    plane_copy(o).wait_send()
                return c

            lax.fori_loop(0, NXZ, sent, 0)
            if s == 0:
                def sent_numer(p, c):
                    numer_copy(p).wait_send()
                    return c

                lax.fori_loop(1, NXZ, sent_numer, 0)

        return drain

    sent_psi = gather(0, psi)
    for k in range(nterms):
        for copy in operator_copies(k):
            copy.wait()
    drain_one = reduce(0)
    psi_float = psi.astype(F32)
    sigma_one = sigma[...] + hdiag[...] * psi_float
    top = jnp.sum(jnp.sum(numer_p[...], axis=0), keepdims=True)
    quotient = top / jnp.sum(denom[...], keepdims=True)
    correction = ((sigma_one - quotient * psi_float) / hdiag[...]).astype(BF16)
    sent_psi()
    sent_correction = gather(1, correction)
    drain_one()
    theta_out[0] = quotient[0, 0]
    pass_lam.wait_send()
    drain_two = reduce(1)
    out[...] = sigma[...] + hdiag[...] * correction.astype(F32)
    sent_correction()
    drain_two()


def body(amat, lam, hdiag, left_ops, right_operators, couple, blockmask):
    terms = left_ops.shape[1]
    vmem, dma = pltpu.VMEM, pltpu.SemaphoreType.DMA
    anywhere = pl.BlockSpec(memory_space=pl.ANY)
    scalars = pl.BlockSpec(memory_space=pltpu.SMEM)
    scratch = [
        vmem((ROWS, BS), BF16), vmem((1, ROWS), F32), vmem((ROWS, BS), F32),
        vmem((terms, NQ, BS, BS), BF16), vmem((terms, NQ, BS, BS), BF16),
        vmem((1, ROWS), F32),
        vmem((2, NQ + 1, BS, BS), BF16),
        vmem((GROUPS, NX, BS, BS), BF16), vmem((2, GROUPS, NX, BS, BS), BF16),
        vmem((2, GROUPS, NX, BS, BS), BF16), vmem((2, 2, GROUPS, NX, BS, BS), BF16),
        vmem((GROUPS, NX, BS, BS), F32), vmem((2, GROUPS, NX, BS, BS), F32),
        vmem((NXZ, ROWS, BS), BF16), vmem((2, NXZ, ROWS, BS), BF16),
        vmem((ROWS, BS), F32),
        vmem((8, BS), F32), vmem((8, BS), F32),
        vmem((NY, 8, BS), F32), vmem((NXZ, 8, BS), F32),
        dma((3,)), dma, dma((2, terms)), dma,
        dma((NXZ,)), dma((2, NXZ)),
        dma((3, NXZ)), dma((3, 2, NXZ)),
        dma((GROUPS,)), dma((2, GROUPS)), dma((2, GROUPS)), dma((2, 2, GROUPS)),
        dma((NXZ,)), dma((2, NXZ)),
        dma((3,)), dma((NY,)),
        dma((NXZ,)), dma((NXZ,)),
    ]
    sigma_two, theta = pl.pallas_call(
        kernel,
        out_shape=(jax.ShapeDtypeStruct((ROWS, BS), F32), jax.ShapeDtypeStruct((1,), F32)),
        in_specs=[anywhere] * 5 + [scalars] * 2,
        out_specs=(pl.BlockSpec(memory_space=pltpu.VMEM), scalars),
        scratch_shapes=scratch,
        compiler_params=pltpu.CompilerParams(collective_id=0, has_side_effects=True),
    )(amat, lam.reshape(1, ROWS), hdiag,
      left_ops.reshape(terms, NQ, BS, BS), right_operators.reshape(terms, NQ, BS, BS),
      couple.reshape(terms, 1, NQ), blockmask.reshape(terms, 1, NQ))
    return sigma_two, theta


def solution(mesh):
    placed = (
        P(("seg", "ops"), None),
        P(("seg", "ops")),
        P(("seg", "ops"), None),
        P("seg", "ops", None, None),
        P("seg", "ops", None, None),
        P("seg", "ops", None),
        P("seg", "ops", None),
    )
    return jax.shard_map(
        body,
        mesh=mesh,
        in_specs=placed,
        out_specs=(P(("seg", "ops"), None), P("seg")),
        check_vma=False,
    )
```

```python
import functools

import jax
import jax.numpy as jnp
from jax import lax
from jax.experimental import pallas as pl
from jax.experimental.pallas import tpu as pltpu
from jax.sharding import PartitionSpec as P

NX, NY, NZ = 2, 4, 8
NXZ = NX * NZ
NSEG = 4
NQ, BS, ROWS = 32, 128, 64
UNIT = GROUPS = 4
CROSS_LAG = 4
F32, BF16 = jnp.float32, jnp.bfloat16


def kernel(amat_h, lam_h, hdiag_h, left_h, right_h, couple, mask,
           out, theta_out,
           amat, lam, hdiag, left, right, lam_in, v, opp_send, near_send,
           opp_in, near_in, own_acc, work, plane_send, plane_in, sigma,
           numer, denom, numer_row, numer_y, numer_p,
           load_sem, lam_sem, op_sem, lam_send, plane_s, plane_r,
           ring_s, ring_r, opp_s, opp_r, near_s, near_r, psum_s, psum_r,
           num_s, num_r, nump_s, nump_r):
    nterms = left.shape[0]
    seg = lax.axis_index("seg")
    me = lax.axis_index("ops")
    x, y, z = me // (NY * NZ), (me // NZ) % NY, me % NZ
    xz = x * NZ + z
    up, down, across = (y + 1) % NY, (y + 3) % NY, (y + 2) % NY

    def device(tx, ty, tz):
        return tx * (NY * NZ) + ty * NZ + tz

    def place(p):
        q = p // 2
        dz = (q % 2) * ((q + 1) // 2) + (1 - q % 2) * (NZ - q // 2)
        return (x + p) % NX, (z + dz) % NZ

    def piece(ref, o):
        return ref.at[o // 2, pl.ds(pl.multiple_of((o % 2) * ROWS, ROWS), ROWS), :]

    def remote(src, dst, s, r, target, axis="ops"):
        return pltpu.make_async_remote_copy(
            src_ref=src, dst_ref=dst, send_sem=s, recv_sem=r,
            device_id={axis: target}, device_id_type=pl.DeviceIdType.MESH)

    small = [pltpu.make_async_copy(amat_h, amat, load_sem.at[0]),
             pltpu.make_async_copy(lam_h, lam, load_sem.at[1]),
             pltpu.make_async_copy(hdiag_h, hdiag, load_sem.at[2])]
    for copy in small:
        copy.start()

    def operator_copies(k):
        return (pltpu.make_async_copy(left_h.at[k], left.at[k], op_sem.at[0, k]),
                pltpu.make_async_copy(right_h.at[k], right.at[k], op_sem.at[1, k]))

    for k in range(nterms):
        for copy in operator_copies(k):
            copy.start()

    barrier = pltpu.get_barrier_semaphore()

    def greet(p, c):
        tx, tz = place(p)
        pl.semaphore_signal(barrier, inc=1, device_id={"ops": device(tx, y, tz)},
                            device_id_type=pl.DeviceIdType.MESH)
        return c

    lax.fori_loop(1, NXZ, greet, 0)
    for other in (up, down, across):
        pl.semaphore_signal(barrier, inc=1, device_id={"ops": device(x, other, z)},
                            device_id_type=pl.DeviceIdType.MESH)
    for step in (1, NSEG - 1):
        pl.semaphore_signal(barrier, inc=1, device_id={"seg": (seg + step) % NSEG},
                            device_id_type=pl.DeviceIdType.MESH)
    for copy in small:
        copy.wait()
    v[0, NQ] = jnp.zeros((BS, BS), BF16)
    v[1, NQ] = jnp.zeros((BS, BS), BF16)
    numer[...] = jnp.zeros_like(numer)
    denom[...] = jnp.zeros_like(denom)
    pl.semaphore_wait(barrier, NXZ - 1 + 3 + 2)

    pass_lam = remote(lam, lam_in, lam_send, lam_sem, (seg + 1) % NSEG, "seg")
    pass_lam.start()
    pass_lam.wait_recv()
    square = (ROWS, ROWS)
    diagonal = lax.broadcasted_iota(jnp.int32, square, 0) == lax.broadcasted_iota(jnp.int32, square, 1)
    earlier = jnp.sum(jnp.where(diagonal, jnp.broadcast_to(lam_in[...], square), 0.0), axis=1, keepdims=True)
    weights = jnp.where(seg == 0, jnp.ones_like(earlier), earlier)
    psi = (weights * amat[...].astype(F32)).astype(BF16)

    mine = (me // 2, pl.ds(pl.multiple_of((me % 2) * ROWS, ROWS), ROWS))

    def gather(s, value):
        vec = v.at[s]
        v[s, mine[0], mine[1], :] = value

        def scatter_copy(p):
            tx, tz = place(p)
            return remote(piece(vec, me), piece(vec, me), plane_s.at[p], plane_r.at[s, xz],
                          device(tx, y, tz))

        def arrival(p, ty, sem):
            tx, tz = place(p)
            where = piece(vec, device(tx, ty, tz))
            return remote(where, where, plane_s.at[p], sem.at[s, tx * NZ + tz], device(x, up, z))

        def pass_up(p):
            tx, tz = place(p)
            where = piece(vec, device(tx, y, tz))
            return remote(where, where, ring_s.at[0, p], ring_r.at[0, s, tx * NZ + tz], device(x, up, z))

        def pass_down(p):
            tx, tz = place(p)
            where = piece(vec, device(tx, y, tz))
            return remote(where, where, ring_s.at[1, p], ring_r.at[1, s, tx * NZ + tz], device(x, down, z))

        def pass_across(p):
            tx, tz = place(p)
            where = piece(vec, device(tx, y, tz))
            return remote(where, where, ring_s.at[2, p], ring_r.at[2, s, tx * NZ + tz], device(x, across, z))

        def cross(n):
            tz = place(2 * n)[1]
            where = piece(vec, device(x, y, tz))
            return remote(where, where, plane_s.at[2 * n + 1], plane_r.at[s, x * NZ + tz], device(1 - x, y, z))

        def first(n, c):
            scatter_copy(2 * n).start()
            return c

        cross(0).start()
        lax.fori_loop(1, NZ, first, 0)

        def fan(p):
            pass_up(p).start()
            pass_down(p).start()
            pass_across(p).start()

        def hop(n, c):
            @pl.when(n < NZ)
            def _():
                @pl.when(n > 0)
                def _():
                    arrival(2 * n, y, plane_r).wait_recv()
                    cross(n).start()
                fan(2 * n)

            @pl.when(n >= CROSS_LAG)
            def _():
                p = 2 * (n - CROSS_LAG) + 1
                arrival(p, y, plane_r).wait_recv()
                fan(p)
            return c

        lax.fori_loop(0, NZ + CROSS_LAG, hop, 0)

        def finish(p, c):
            arrival(p, down, ring_r.at[0]).wait_recv()
            arrival(p, up, ring_r.at[1]).wait_recv()
            arrival(p, across, ring_r.at[2]).wait_recv()
            return c

        lax.fori_loop(0, NXZ, finish, 0)

        def sent(p, c):
            @pl.when(p > 0)
            def _():
                scatter_copy(p).wait_send()
            pass_up(p).wait_send()
            pass_down(p).wait_send()
            pass_across(p).wait_send()
            return c

        return functools.partial(lax.fori_loop, 0, NXZ, sent, 0)

    contract = (((1,), (1,)), ((), ()))

    def block(s, i):
        inner = []
        for k in range(nterms):
            live = mask[k, 0, i]
            j = couple[k, 0, i] * live + NQ * (1 - live)
            inner.append(jnp.dot(left[k, i], v[s, j], preferred_element_type=F32).astype(BF16))
        total = None
        for k in range(0, nterms, 2):
            pair = jnp.concatenate(inner[k:k + 2], axis=1)
            rpair = jnp.concatenate([right[k, i], right[k + 1, i]], axis=1)
            part = lax.dot_general(pair, rpair, contract, preferred_element_type=F32)
            total = part if total is None else total + part
        if s == 0:
            here = v[s, i].astype(F32)
            numer[...] += jnp.sum((total * here).reshape(BS // 8, 8, BS), axis=0)
            denom[...] += jnp.sum((here * here).reshape(BS // 8, 8, BS), axis=0)
        return total

    def block_of(half, ty, g):
        return half * (NQ // 2) + ty * UNIT + (z // 2 + (2 - g) * (g < 2) + 3 * (g == 2)) % UNIT

    def unit(s, ty, g):
        return [block(s, block_of(half, ty, g)) for half in range(NX)]

    def reduce(s):
        def opp_copy(g):
            target = device(x, (y + 1 + 2 * (g % 2)) % NY, z)
            return remote(opp_send.at[g], opp_in.at[s, g], opp_s.at[g], opp_r.at[s, g], target)

        def near_copy(d, g):
            target = device(x, (y + 1 + 2 * d) % NY, z)
            return remote(near_send.at[d, g], near_in.at[s, d, g], near_s.at[d, g], near_r.at[s, d, g], target)

        def opposite(n, c):
            groups = tuple(range(GROUPS))
            totals = [unit(s, across, g) for g in groups]
            for g, both in zip(groups, totals):
                for half in range(NX):
                    opp_send[g, half] = both[half].astype(BF16)
                opp_copy(g).start()
            return c

        lax.fori_loop(0, 1, opposite, 0)

        def passed(g):
            d = g % 2
            opp_copy(g).wait_recv()
            for half in range(NX):
                near_send[d, g, half] = (work[d, g, half] + opp_in[s, g, half].astype(F32)).astype(BF16)
            near_copy(d, g).start()

        def near(n, c):
            totals = [[unit(s, other, 2 * n + e) for other in (up, down)] for e in range(2)]
            for e in range(2):
                g = 2 * n + e
                for half in range(NX):
                    work[e, g, half] = totals[e][e][half]
                    near_send[1 - e, g, half] = totals[e][1 - e][half].astype(BF16)
                near_copy(1 - e, g).start()

            @pl.when(n >= 1)
            def _():
                passed(0)
                passed(1)
            return c

        lax.fori_loop(0, GROUPS // 2, near, 0)

        def plane_copy(o):
            return remote(plane_send.at[o], plane_in.at[s, xz], psum_s.at[o], psum_r.at[s, xz],
                          device(o // NZ, y, o % NZ))

        def pass_on(g):
            for d in range(2):
                near_copy(d, g).wait_recv()
            first = block_of(0, 0, g)
            for half in range(NX):
                total = own_acc[g, half] + near_in[s, 0, g, half].astype(F32) + near_in[s, 1, g, half].astype(F32)
                own_acc[g, half] = total
                for side in range(2):
                    plane_send[half * NZ + 2 * first + side] = total[side * ROWS:(side + 1) * ROWS].astype(BF16)
            for half in range(NX):
                for side in range(2):
                    o = half * NZ + 2 * first + side

                    @pl.when(o != xz)
                    def _():
                        plane_copy(o).start()

        def own(n, c):
            groups = tuple(range(GROUPS))
            totals = [unit(s, y, g) for g in groups]
            for g, both in zip(groups, totals):
                for half in range(NX):
                    own_acc[g, half] = both[half]
            passed(2)
            passed(3)
            return c

        lax.fori_loop(0, 1, own, 0)

        sends = []
        if s == 0:
            start = psi.astype(F32)
            numer[...] += jnp.sum((hdiag[...] * start * start).reshape(ROWS // 8, 8, BS), axis=0)
            numer_row[...] = jnp.sum(numer[...], axis=0, keepdims=True)
            numer_y[y] = numer_row[...]
            for n, other in enumerate((up, down, across)):
                copy = remote(numer_row, numer_y.at[y], num_s.at[n], num_r.at[y], device(x, other, z))
                copy.start()
                sends.append(copy)

        lax.fori_loop(0, GROUPS // 2, lambda g, c: (pass_on(g), c)[1], 0)

        if s == 0:
            for other in (up, down, across):
                remote(numer_row, numer_y.at[other], num_s.at[0], num_r.at[other], device(x, up, z)).wait_recv()
            numer_p[xz] = (numer_y[0] + numer_y[1]) + (numer_y[2] + numer_y[3])

            def numer_copy(p):
                tx, tz = place(p)
                return remote(numer_p.at[xz], numer_p.at[xz], nump_s.at[p], nump_r.at[xz], device(tx, y, tz))

            def go_numer(p, c):
                numer_copy(p).start()
                return c

            lax.fori_loop(1, NXZ, go_numer, 0)

        lax.fori_loop(GROUPS // 2, GROUPS, lambda g, c: (pass_on(g), c)[1], 0)

        sigma[...] = own_acc[GROUPS - 1, x, pl.ds(pl.multiple_of((z % 2) * ROWS, ROWS), ROWS), :]

        def take(p, c):
            tx, tz = place(p)
            o = tx * NZ + tz
            remote(plane_in.at[s, o], plane_in.at[s, o], psum_s.at[0], psum_r.at[s, o],
                   device(x, up, z)).wait_recv()
            sigma[...] += plane_in[s, o].astype(F32)
            return c

        lax.fori_loop(1, NXZ, take, 0)

        if s == 0:
            def take_numer(p, c):
                tx, tz = place(p)
                o = tx * NZ + tz
                remote(numer_p.at[o], numer_p.at[o], nump_s.at[0], nump_r.at[o], device(x, up, z)).wait_recv()
                return c

            lax.fori_loop(1, NXZ, take_numer, 0)

        def drain():
            for copy in sends:
                copy.wait_send()

            def sent_ring(g, c):
                opp_copy(g).wait_send()
                near_copy(0, g).wait_send()
                near_copy(1, g).wait_send()
                return c

            lax.fori_loop(0, GROUPS, sent_ring, 0)

            def sent(o, c):
                @pl.when(o != xz)
                def _():
                    plane_copy(o).wait_send()
                return c

            lax.fori_loop(0, NXZ, sent, 0)
            if s == 0:
                def sent_numer(p, c):
                    numer_copy(p).wait_send()
                    return c

                lax.fori_loop(1, NXZ, sent_numer, 0)

        return drain

    sent_psi = gather(0, psi)
    for k in range(nterms):
        for copy in operator_copies(k):
            copy.wait()
    drain_one = reduce(0)
    psi_float = psi.astype(F32)
    sigma_one = sigma[...] + hdiag[...] * psi_float
    top = jnp.sum(jnp.sum(numer_p[...], axis=0), keepdims=True)
    quotient = top / jnp.sum(denom[...], keepdims=True)
    correction = ((sigma_one - quotient * psi_float) / hdiag[...]).astype(BF16)
    sent_psi()
    sent_correction = gather(1, correction)
    drain_one()
    theta_out[0] = quotient[0, 0]
    pass_lam.wait_send()
    drain_two = reduce(1)
    out[...] = sigma[...] + hdiag[...] * correction.astype(F32)
    sent_correction()
    drain_two()


def body(amat, lam, hdiag, left_ops, right_operators, couple, blockmask):
    terms = left_ops.shape[1]
    vmem, dma = pltpu.VMEM, pltpu.SemaphoreType.DMA
    anywhere = pl.BlockSpec(memory_space=pl.ANY)
    scalars = pl.BlockSpec(memory_space=pltpu.SMEM)
    scratch = [
        vmem((ROWS, BS), BF16), vmem((1, ROWS), F32), vmem((ROWS, BS), F32),
        vmem((terms, NQ, BS, BS), BF16), vmem((terms, NQ, BS, BS), BF16),
        vmem((1, ROWS), F32),
        vmem((2, NQ + 1, BS, BS), BF16),
        vmem((GROUPS, NX, BS, BS), BF16), vmem((2, GROUPS, NX, BS, BS), BF16),
        vmem((2, GROUPS, NX, BS, BS), BF16), vmem((2, 2, GROUPS, NX, BS, BS), BF16),
        vmem((GROUPS, NX, BS, BS), F32), vmem((2, GROUPS, NX, BS, BS), F32),
        vmem((NXZ, ROWS, BS), BF16), vmem((2, NXZ, ROWS, BS), BF16),
        vmem((ROWS, BS), F32),
        vmem((8, BS), F32), vmem((8, BS), F32),
        vmem((1, BS), F32), vmem((NY, 1, BS), F32), vmem((NXZ, 1, BS), F32),
        dma((3,)), dma, dma((2, terms)), dma,
        dma((NXZ,)), dma((2, NXZ)),
        dma((3, NXZ)), dma((3, 2, NXZ)),
        dma((GROUPS,)), dma((2, GROUPS)), dma((2, GROUPS)), dma((2, 2, GROUPS)),
        dma((NXZ,)), dma((2, NXZ)),
        dma((3,)), dma((NY,)),
        dma((NXZ,)), dma((NXZ,)),
    ]
    sigma_two, theta = pl.pallas_call(
        kernel,
        out_shape=(jax.ShapeDtypeStruct((ROWS, BS), F32), jax.ShapeDtypeStruct((1,), F32)),
        in_specs=[anywhere] * 5 + [scalars] * 2,
        out_specs=(pl.BlockSpec(memory_space=pltpu.VMEM), scalars),
        scratch_shapes=scratch,
        compiler_params=pltpu.CompilerParams(collective_id=0, has_side_effects=True),
    )(amat, lam.reshape(1, ROWS), hdiag,
      left_ops.reshape(terms, NQ, BS, BS), right_operators.reshape(terms, NQ, BS, BS),
      couple.reshape(terms, 1, NQ), blockmask.reshape(terms, 1, NQ))
    return sigma_two, theta


def solution(mesh):
    placed = (
        P(("seg", "ops"), None),
        P(("seg", "ops")),
        P(("seg", "ops"), None),
        P("seg", "ops", None, None),
        P("seg", "ops", None, None),
        P("seg", "ops", None),
        P("seg", "ops", None),
    )
    return jax.shard_map(
        body,
        mesh=mesh,
        in_specs=placed,
        out_specs=(P(("seg", "ops"), None), P("seg")),
        check_vma=False,
    )
```

```python
import functools

import jax
import jax.numpy as jnp
from jax import lax
from jax.experimental import pallas as pl
from jax.experimental.pallas import tpu as pltpu
from jax.sharding import PartitionSpec as P

NX, NY, NZ = 2, 4, 8
NXZ = NX * NZ
NSEG = 4
NQ, BS, ROWS = 32, 128, 64
UNIT = GROUPS = 4
CROSS_LAG = 4
F32, BF16 = jnp.float32, jnp.bfloat16


def kernel(amat_h, lam_h, hdiag_h, left_h, right_h, couple, mask,
           out, theta_out,
           amat, lam, hdiag, left, right, lam_in, v, opp_send, near_send,
           opp_in, near_in, own_acc, work, plane_send, plane_in, sigma,
           numer, denom, numer_row, numer_y, numer_p,
           load_sem, lam_sem, op_sem, lam_send, plane_s, plane_r,
           ring_s, ring_r, opp_s, opp_r, near_s, near_r, psum_s, psum_r,
           num_s, num_r, nump_s, nump_r):
    nterms = left.shape[0]
    seg = lax.axis_index("seg")
    me = lax.axis_index("ops")
    x, y, z = me // (NY * NZ), (me // NZ) % NY, me % NZ
    xz = x * NZ + z
    up, down, across = (y + 1) % NY, (y + 3) % NY, (y + 2) % NY

    def device(tx, ty, tz):
        return tx * (NY * NZ) + ty * NZ + tz

    def place(p):
        q = p // 2
        dz = (q % 2) * ((q + 1) // 2) + (1 - q % 2) * (NZ - q // 2)
        return (x + p) % NX, (z + dz) % NZ

    def piece(ref, o):
        return ref.at[o // 2, pl.ds(pl.multiple_of((o % 2) * ROWS, ROWS), ROWS), :]

    def remote(src, dst, s, r, target, axis="ops"):
        return pltpu.make_async_remote_copy(
            src_ref=src, dst_ref=dst, send_sem=s, recv_sem=r,
            device_id={axis: target}, device_id_type=pl.DeviceIdType.MESH)

    small = [pltpu.make_async_copy(amat_h, amat, load_sem.at[0]),
             pltpu.make_async_copy(lam_h, lam, load_sem.at[1]),
             pltpu.make_async_copy(hdiag_h, hdiag, load_sem.at[2])]
    for copy in small:
        copy.start()

    def operator_copies(k):
        return (pltpu.make_async_copy(left_h.at[k], left.at[k], op_sem.at[0, k]),
                pltpu.make_async_copy(right_h.at[k], right.at[k], op_sem.at[1, k]))

    for k in range(nterms):
        for copy in operator_copies(k):
            copy.start()

    barrier = pltpu.get_barrier_semaphore()

    def greet(p, c):
        tx, tz = place(p)
        pl.semaphore_signal(barrier, inc=1, device_id={"ops": device(tx, y, tz)},
                            device_id_type=pl.DeviceIdType.MESH)
        return c

    lax.fori_loop(1, NXZ, greet, 0)
    for other in (up, down, across):
        pl.semaphore_signal(barrier, inc=1, device_id={"ops": device(x, other, z)},
                            device_id_type=pl.DeviceIdType.MESH)
    for step in (1, NSEG - 1):
        pl.semaphore_signal(barrier, inc=1, device_id={"seg": (seg + step) % NSEG},
                            device_id_type=pl.DeviceIdType.MESH)
    for copy in small:
        copy.wait()
    v[0, NQ] = jnp.zeros((BS, BS), BF16)
    v[1, NQ] = jnp.zeros((BS, BS), BF16)
    numer[...] = jnp.zeros_like(numer)
    denom[...] = jnp.zeros_like(denom)
    pl.semaphore_wait(barrier, NXZ - 1 + 3 + 2)

    pass_lam = remote(lam, lam_in, lam_send, lam_sem, (seg + 1) % NSEG, "seg")
    pass_lam.start()
    pass_lam.wait_recv()
    square = (ROWS, ROWS)
    diagonal = lax.broadcasted_iota(jnp.int32, square, 0) == lax.broadcasted_iota(jnp.int32, square, 1)
    earlier = jnp.sum(jnp.where(diagonal, jnp.broadcast_to(lam_in[...], square), 0.0), axis=1, keepdims=True)
    weights = jnp.where(seg == 0, jnp.ones_like(earlier), earlier)
    psi = (weights * amat[...].astype(F32)).astype(BF16)

    mine = (me // 2, pl.ds(pl.multiple_of((me % 2) * ROWS, ROWS), ROWS))

    def gather(s, value):
        vec = v.at[s]
        v[s, mine[0], mine[1], :] = value

        def scatter_copy(p):
            tx, tz = place(p)
            return remote(piece(vec, me), piece(vec, me), plane_s.at[p], plane_r.at[s, xz],
                          device(tx, y, tz))

        def arrival(p, ty, sem):
            tx, tz = place(p)
            where = piece(vec, device(tx, ty, tz))
            return remote(where, where, plane_s.at[p], sem.at[s, tx * NZ + tz], device(x, up, z))

        def pass_up(p):
            tx, tz = place(p)
            where = piece(vec, device(tx, y, tz))
            return remote(where, where, ring_s.at[0, p], ring_r.at[0, s, tx * NZ + tz], device(x, up, z))

        def pass_down(p):
            tx, tz = place(p)
            where = piece(vec, device(tx, y, tz))
            return remote(where, where, ring_s.at[1, p], ring_r.at[1, s, tx * NZ + tz], device(x, down, z))

        def pass_across(p):
            tx, tz = place(p)
            where = piece(vec, device(tx, y, tz))
            return remote(where, where, ring_s.at[2, p], ring_r.at[2, s, tx * NZ + tz], device(x, across, z))

        def cross(n):
            tz = place(2 * n)[1]
            where = piece(vec, device(x, y, tz))
            return remote(where, where, plane_s.at[2 * n + 1], plane_r.at[s, x * NZ + tz], device(1 - x, y, z))

        def first(n, c):
            scatter_copy(2 * n).start()
            return c

        cross(0).start()
        lax.fori_loop(1, NZ, first, 0)

        def fan(p):
            pass_across(p).start()
            pass_up(p).start()
            pass_down(p).start()

        def hop(n, c):
            @pl.when(n < NZ)
            def _():
                @pl.when(n > 0)
                def _():
                    arrival(2 * n, y, plane_r).wait_recv()
                    cross(n).start()
                fan(2 * n)

            @pl.when(n >= CROSS_LAG)
            def _():
                p = 2 * (n - CROSS_LAG) + 1
                arrival(p, y, plane_r).wait_recv()
                fan(p)
            return c

        lax.fori_loop(0, NZ + CROSS_LAG, hop, 0)

        def finish(p, c):
            arrival(p, down, ring_r.at[0]).wait_recv()
            arrival(p, up, ring_r.at[1]).wait_recv()
            arrival(p, across, ring_r.at[2]).wait_recv()
            return c

        lax.fori_loop(0, NXZ, finish, 0)

        def sent(p, c):
            @pl.when(p > 0)
            def _():
                scatter_copy(p).wait_send()
            pass_up(p).wait_send()
            pass_down(p).wait_send()
            pass_across(p).wait_send()
            return c

        return functools.partial(lax.fori_loop, 0, NXZ, sent, 0)

    contract = (((1,), (1,)), ((), ()))

    def block(s, i):
        inner = []
        for k in range(nterms):
            live = mask[k, 0, i]
            j = couple[k, 0, i] * live + NQ * (1 - live)
            inner.append(jnp.dot(left[k, i], v[s, j], preferred_element_type=F32).astype(BF16))
        total = None
        for k in range(0, nterms, 2):
            pair = jnp.concatenate(inner[k:k + 2], axis=1)
            rpair = jnp.concatenate([right[k, i], right[k + 1, i]], axis=1)
            part = lax.dot_general(pair, rpair, contract, preferred_element_type=F32)
            total = part if total is None else total + part
        if s == 0:
            here = v[s, i].astype(F32)
            numer[...] += jnp.sum((total * here).reshape(BS // 8, 8, BS), axis=0)
            denom[...] += jnp.sum((here * here).reshape(BS // 8, 8, BS), axis=0)
        return total

    def block_of(half, ty, g):
        return half * (NQ // 2) + ty * UNIT + (z // 2 + (2 - g) * (g < 2) + 3 * (g == 2)) % UNIT

    def unit(s, ty, g):
        return [block(s, block_of(half, ty, g)) for half in range(NX)]

    def reduce(s):
        def opp_copy(g):
            target = device(x, (y + 1 + 2 * (g % 2)) % NY, z)
            return remote(opp_send.at[g], opp_in.at[s, g], opp_s.at[g], opp_r.at[s, g], target)

        def near_copy(d, g):
            target = device(x, (y + 1 + 2 * d) % NY, z)
            return remote(near_send.at[d, g], near_in.at[s, d, g], near_s.at[d, g], near_r.at[s, d, g], target)

        def opposite(n, c):
            groups = tuple(range(GROUPS))
            totals = [unit(s, across, g) for g in groups]
            for g, both in zip(groups, totals):
                for half in range(NX):
                    opp_send[g, half] = both[half].astype(BF16)
                opp_copy(g).start()
            return c

        lax.fori_loop(0, 1, opposite, 0)

        def passed(g):
            d = g % 2
            opp_copy(g).wait_recv()
            for half in range(NX):
                near_send[d, g, half] = (work[d, g, half] + opp_in[s, g, half].astype(F32)).astype(BF16)
            near_copy(d, g).start()

        def near(n, c):
            totals = [[unit(s, other, 2 * n + e) for other in (up, down)] for e in range(2)]
            for e in range(2):
                g = 2 * n + e
                for half in range(NX):
                    work[e, g, half] = totals[e][e][half]
                    near_send[1 - e, g, half] = totals[e][1 - e][half].astype(BF16)
                near_copy(1 - e, g).start()

            @pl.when(n >= 1)
            def _():
                passed(0)
                passed(1)
            return c

        lax.fori_loop(0, GROUPS // 2, near, 0)

        def plane_copy(o):
            return remote(plane_send.at[o], plane_in.at[s, xz], psum_s.at[o], psum_r.at[s, xz],
                          device(o // NZ, y, o % NZ))

        def pass_on(g):
            for d in range(2):
                near_copy(d, g).wait_recv()
            first = block_of(0, 0, g)
            for half in range(NX):
                total = own_acc[g, half] + near_in[s, 0, g, half].astype(F32) + near_in[s, 1, g, half].astype(F32)
                own_acc[g, half] = total
                for side in range(2):
                    plane_send[half * NZ + 2 * first + side] = total[side * ROWS:(side + 1) * ROWS].astype(BF16)
            for half in range(NX):
                for side in range(2):
                    o = half * NZ + 2 * first + side

                    @pl.when(o != xz)
                    def _():
                        plane_copy(o).start()

        def own(n, c):
            groups = tuple(range(GROUPS))
            totals = [unit(s, y, g) for g in groups]
            for g, both in zip(groups, totals):
                for half in range(NX):
                    own_acc[g, half] = both[half]
            passed(2)
            passed(3)
            return c

        lax.fori_loop(0, 1, own, 0)

        sends = []
        if s == 0:
            start = psi.astype(F32)
            numer[...] += jnp.sum((hdiag[...] * start * start).reshape(ROWS // 8, 8, BS), axis=0)
            numer_row[...] = jnp.sum(numer[...], axis=0, keepdims=True)
            numer_y[y] = numer_row[...]
            for n, other in enumerate((up, down, across)):
                copy = remote(numer_row, numer_y.at[y], num_s.at[n], num_r.at[y], device(x, other, z))
                copy.start()
                sends.append(copy)

        lax.fori_loop(0, GROUPS // 2, lambda g, c: (pass_on(g), c)[1], 0)

        if s == 0:
            for other in (up, down, across):
                remote(numer_row, numer_y.at[other], num_s.at[0], num_r.at[other], device(x, up, z)).wait_recv()
            numer_p[xz] = (numer_y[0] + numer_y[1]) + (numer_y[2] + numer_y[3])

            def numer_copy(p):
                tx, tz = place(p)
                return remote(numer_p.at[xz], numer_p.at[xz], nump_s.at[p], nump_r.at[xz], device(tx, y, tz))

            def go_numer(p, c):
                numer_copy(p).start()
                return c

            lax.fori_loop(1, NXZ, go_numer, 0)

        lax.fori_loop(GROUPS // 2, GROUPS, lambda g, c: (pass_on(g), c)[1], 0)

        sigma[...] = own_acc[GROUPS - 1, x, pl.ds(pl.multiple_of((z % 2) * ROWS, ROWS), ROWS), :]

        def take(p, c):
            tx, tz = place(p)
            o = tx * NZ + tz
            remote(plane_in.at[s, o], plane_in.at[s, o], psum_s.at[0], psum_r.at[s, o],
                   device(x, up, z)).wait_recv()
            sigma[...] += plane_in[s, o].astype(F32)
            return c

        lax.fori_loop(1, NXZ, take, 0)

        if s == 0:
            def take_numer(p, c):
                tx, tz = place(p)
                o = tx * NZ + tz
                remote(numer_p.at[o], numer_p.at[o], nump_s.at[0], nump_r.at[o], device(x, up, z)).wait_recv()
                return c

            lax.fori_loop(1, NXZ, take_numer, 0)

        def drain():
            for copy in sends:
                copy.wait_send()

            def sent_ring(g, c):
                opp_copy(g).wait_send()
                near_copy(0, g).wait_send()
                near_copy(1, g).wait_send()
                return c

            lax.fori_loop(0, GROUPS, sent_ring, 0)

            def sent(o, c):
                @pl.when(o != xz)
                def _():
                    plane_copy(o).wait_send()
                return c

            lax.fori_loop(0, NXZ, sent, 0)
            if s == 0:
                def sent_numer(p, c):
                    numer_copy(p).wait_send()
                    return c

                lax.fori_loop(1, NXZ, sent_numer, 0)

        return drain

    sent_psi = gather(0, psi)
    for k in range(nterms):
        for copy in operator_copies(k):
            copy.wait()
    drain_one = reduce(0)
    psi_float = psi.astype(F32)
    sigma_one = sigma[...] + hdiag[...] * psi_float
    top = jnp.sum(jnp.sum(numer_p[...], axis=0), keepdims=True)
    quotient = top / jnp.sum(denom[...], keepdims=True)
    correction = ((sigma_one - quotient * psi_float) / hdiag[...]).astype(BF16)
    sent_psi()
    sent_correction = gather(1, correction)
    drain_one()
    theta_out[0] = quotient[0, 0]
    pass_lam.wait_send()
    drain_two = reduce(1)
    out[...] = sigma[...] + hdiag[...] * correction.astype(F32)
    sent_correction()
    drain_two()


def body(amat, lam, hdiag, left_ops, right_operators, couple, blockmask):
    terms = left_ops.shape[1]
    vmem, dma = pltpu.VMEM, pltpu.SemaphoreType.DMA
    anywhere = pl.BlockSpec(memory_space=pl.ANY)
    scalars = pl.BlockSpec(memory_space=pltpu.SMEM)
    scratch = [
        vmem((ROWS, BS), BF16), vmem((1, ROWS), F32), vmem((ROWS, BS), F32),
        vmem((terms, NQ, BS, BS), BF16), vmem((terms, NQ, BS, BS), BF16),
        vmem((1, ROWS), F32),
        vmem((2, NQ + 1, BS, BS), BF16),
        vmem((GROUPS, NX, BS, BS), BF16), vmem((2, GROUPS, NX, BS, BS), BF16),
        vmem((2, GROUPS, NX, BS, BS), BF16), vmem((2, 2, GROUPS, NX, BS, BS), BF16),
        vmem((GROUPS, NX, BS, BS), F32), vmem((2, GROUPS, NX, BS, BS), F32),
        vmem((NXZ, ROWS, BS), BF16), vmem((2, NXZ, ROWS, BS), BF16),
        vmem((ROWS, BS), F32),
        vmem((8, BS), F32), vmem((8, BS), F32),
        vmem((1, BS), F32), vmem((NY, 1, BS), F32), vmem((NXZ, 1, BS), F32),
        dma((3,)), dma, dma((2, terms)), dma,
        dma((NXZ,)), dma((2, NXZ)),
        dma((3, NXZ)), dma((3, 2, NXZ)),
        dma((GROUPS,)), dma((2, GROUPS)), dma((2, GROUPS)), dma((2, 2, GROUPS)),
        dma((NXZ,)), dma((2, NXZ)),
        dma((3,)), dma((NY,)),
        dma((NXZ,)), dma((NXZ,)),
    ]
    sigma_two, theta = pl.pallas_call(
        kernel,
        out_shape=(jax.ShapeDtypeStruct((ROWS, BS), F32), jax.ShapeDtypeStruct((1,), F32)),
        in_specs=[anywhere] * 5 + [scalars] * 2,
        out_specs=(pl.BlockSpec(memory_space=pltpu.VMEM), scalars),
        scratch_shapes=scratch,
        compiler_params=pltpu.CompilerParams(collective_id=0, has_side_effects=True),
    )(amat, lam.reshape(1, ROWS), hdiag,
      left_ops.reshape(terms, NQ, BS, BS), right_operators.reshape(terms, NQ, BS, BS),
      couple.reshape(terms, 1, NQ), blockmask.reshape(terms, 1, NQ))
    return sigma_two, theta


def solution(mesh):
    placed = (
        P(("seg", "ops"), None),
        P(("seg", "ops")),
        P(("seg", "ops"), None),
        P("seg", "ops", None, None),
        P("seg", "ops", None, None),
        P("seg", "ops", None),
        P("seg", "ops", None),
    )
    return jax.shard_map(
        body,
        mesh=mesh,
        in_specs=placed,
        out_specs=(P(("seg", "ops"), None), P("seg")),
        check_vma=False,
    )
```
